32 devices in a mesh: seq: 4 (over y, x), exp: 8 (over z, core).
Axes of the slice: x: 2, y: 2, z: 4, core: 2. Of those that a mesh axis runs over, the one named last changes fastest.
Arguments:
- tokens: bfloat16 [2, 24576, 1024], P(None, ('seq', 'exp')), may hold values from -60 to 60
- router: bfloat16 [1024, 64], replicated, may hold values from -0.25 to 0.25
- w_in: bfloat16 [16, 1024, 4096], P('exp', None, 'seq'), may hold values from -0.1875 to 0.1875
- w_out: bfloat16 [16, 4096, 1024], P('exp', 'seq'), may hold values from -0.09375 to 0.09375
- grad_out: bfloat16 [2, 24576, 1024], P(None, ('seq', 'exp')), may hold values from -6 to 6
Outputs:
- mixed: bfloat16 [2, 24576, 1024], P(None, ('seq', 'exp'))
- grad_tokens: bfloat16 [2, 24576, 1024], P(None, ('seq', 'exp'))
- grad_router: float32 [1024, 64], P(('seq', 'exp'))
- grad_w_in: bfloat16 [16, 1024, 4096], P('exp', None, 'seq')
- grad_w_out: bfloat16 [16, 4096, 1024], P('exp', 'seq')
The draws below stay inside these ranges and needn't reach their ends.
All inputs are finite; a program needn't handle non-finite values.
Results may differ from the reference program's by a relative error of at most 0.018.
Values may be sent and summed in bfloat16 or wider, within the bound.
A program may use at most 128 MiB of HBM per device.

```python
import math
import jax
import jax.numpy as jnp
from jax import lax

D = 1024
FF = 4096
SLOTS = 4
CLIPS = 2
EXPERTS = 16
SLOT_COUNT = 64
TOKENS = 24576


def router_base(key):
    base = jax.random.normal(jax.random.fold_in(key, 7), (D, SLOT_COUNT), jnp.float32) / math.sqrt(D)
    return jnp.clip(base, -0.25, 0.25)


def draw_router(key, part):
    return router_base(key).astype(jnp.bfloat16)


def draw_tokens(key, part):
    values = jax.random.normal(jax.random.fold_in(key, 11), (CLIPS, TOKENS, D), jnp.float32)
    return jnp.clip(values, -6.0, 6.0).astype(jnp.bfloat16)


def block_levels(key, shape, split, least, top_value):
    def one(dim, blocks):
        steps = jax.random.uniform(jax.random.fold_in(jax.random.fold_in(key, 6), dim), (blocks,), jnp.float32, least / len(split), top_value / len(split))
        return jnp.repeat(jnp.exp(steps), shape[dim] // blocks).reshape((-1,) + (1,) * (len(shape) - dim - 1))

    loudness = one(*split[0])
    for cut in split[1:]:
        loudness = loudness * one(*cut)
    return loudness


def gaussian(stream_key, dims, spread, limit, split=(), kind=jnp.bfloat16):
    gain = block_levels(stream_key, dims, split, -0.22, 0.18) if split else 1.0
    array = jax.random.normal(stream_key, dims, jnp.float32) * spread * gain
    return jnp.minimum(jnp.maximum(array, -limit), limit).astype(kind)


def setup_inputs(seed: int = 0) -> dict:
    keys = jax.random.split(jax.random.key(seed), 6)
    return {
        "tokens": draw_tokens(jax.random.fold_in(keys[5], 71), 0),
        "router": draw_router(jax.random.fold_in(keys[5], 71), 0),
        "w_in": gaussian(keys[2], (EXPERTS, D, FF), D ** -0.5, 0.1875, ((0, 8), (2, 4))),
        "w_out": gaussian(keys[3], (EXPERTS, FF, D), FF ** -0.5, 0.09375, ((0, 8), (1, 4))),
        "grad_out": gaussian(keys[4], (CLIPS, TOKENS, D), 1.0, 6.0, ((1, 32),)),
    }


def reference(tokens, router, w_in, w_out, grad_out):
    width = tokens.shape[2]
    slot_total = router.shape[1]
    experts = w_in.shape[0]
    tokens_f = tokens.astype(jnp.float32)
    grad_f = grad_out.astype(jnp.float32)
    logits = jnp.dot(tokens.reshape(CLIPS * TOKENS, width).astype(jnp.float32), router.astype(jnp.float32), preferred_element_type=jnp.float32).reshape(CLIPS, TOKENS, slot_total)
    slot_peak = lax.optimization_barrier(jnp.max(logits, axis=1, keepdims=True))
    exp_terms = jnp.exp(logits - slot_peak)
    dispatch = exp_terms / lax.optimization_barrier(jnp.sum(exp_terms, axis=1, keepdims=True))
    dispatch_b = dispatch.astype(jnp.bfloat16)
    mixing = jax.nn.softmax(logits, axis=2)
    mixing_b = mixing.astype(jnp.bfloat16)
    slot_in = jnp.einsum('cts,ctd->scd', dispatch_b.astype(jnp.float32), tokens_f).astype(jnp.bfloat16)
    expert_rows = slot_in.reshape(experts, SLOTS * CLIPS, width)
    pre = jnp.einsum('erd,edh->erh', expert_rows.astype(jnp.float32), w_in.astype(jnp.float32))
    hidden = jax.nn.gelu(pre).astype(jnp.bfloat16)
    slot_out = jnp.einsum('erh,ehd->erd', hidden.astype(jnp.float32), w_out.astype(jnp.float32)).astype(jnp.bfloat16)
    slot_out = slot_out.reshape(slot_total, CLIPS, width)
    slot_out_f = slot_out.astype(jnp.float32)
    mixed = jnp.einsum('cts,scd->ctd', mixing_b.astype(jnp.float32), slot_out_f).astype(jnp.bfloat16)
    mixing_grad = jnp.einsum('ctd,scd->cts', grad_f, slot_out_f)
    slot_grad = jnp.einsum('cts,ctd->scd', mixing_b.astype(jnp.float32), grad_f).astype(jnp.bfloat16)
    grad_rows = slot_grad.reshape(experts, SLOTS * CLIPS, width).astype(jnp.float32)
    hidden_grad = jnp.einsum('erd,ehd->erh', grad_rows, w_out.astype(jnp.float32))
    pre_grad = jax.vjp(jax.nn.gelu, pre)[1](hidden_grad)[0].astype(jnp.bfloat16)
    pre_grad_f = pre_grad.astype(jnp.float32)
    grad_w_out = jnp.einsum('erh,erd->ehd', hidden.astype(jnp.float32), grad_rows).astype(jnp.bfloat16)
    grad_w_in = jnp.einsum('erd,erh->edh', expert_rows.astype(jnp.float32), pre_grad_f).astype(jnp.bfloat16)
    slot_in_grad = jnp.einsum('erh,edh->erd', pre_grad_f, w_in.astype(jnp.float32)).astype(jnp.bfloat16)
    slot_in_grad = slot_in_grad.reshape(slot_total, CLIPS, width).astype(jnp.float32)
    dispatch_grad = jnp.einsum('ctd,scd->cts', tokens_f, slot_in_grad)
    inner = lax.optimization_barrier(jnp.sum(dispatch * dispatch_grad, axis=1, keepdims=True))
    logit_grad = dispatch * (dispatch_grad - inner) + mixing * (mixing_grad - lax.optimization_barrier(jnp.sum(mixing * mixing_grad, axis=2, keepdims=True)))
    logit_b = logit_grad.astype(jnp.bfloat16)
    token_part = jnp.einsum('cts,scd->ctd', dispatch_b.astype(jnp.float32), slot_in_grad)
    router_part = jnp.dot(logit_b.reshape(CLIPS * TOKENS, slot_total).astype(jnp.float32), router.T.astype(jnp.float32), preferred_element_type=jnp.float32).reshape(CLIPS, TOKENS, width)
    grad_tokens = (token_part + router_part).astype(jnp.bfloat16)
    grad_router = jnp.einsum('ctd,cts->ds', tokens_f, logit_b.astype(jnp.float32))
    return (mixed, grad_tokens, grad_router, grad_w_in, grad_w_out)
```

```python
import functools

import jax
import jax.numpy as jnp
from jax import lax
from jax.experimental import pallas as pl
from jax.experimental.pallas import tpu as pltpu
from jax.sharding import PartitionSpec as P

MESH = pl.DeviceIdType.MESH
F32 = jnp.float32
BF16 = jnp.bfloat16
NT = (((1,), (1,)), ((), ()))


def dot(a, b):
    return jnp.dot(a, b, preferred_element_type=F32)


def dot_nt(a, b):
    return lax.dot_general(a, b, NT, preferred_element_type=F32)


def place(seq_n, exp_n):
    s = lax.axis_index("seq")
    e = lax.axis_index("exp")
    h, par = e // 2, e % 2
    pair = (s, h * 2 + (1 - par))
    seq_peers = [((s + k) % seq_n, e) for k in range(1, seq_n)]
    exp_peers = [(s, ((h + k) % (exp_n // 2)) * 2 + par) for k in range(1, exp_n // 2)]
    return s, h, par, pair, seq_peers, exp_peers


def greet(peers):
    barrier = pltpu.get_barrier_semaphore()
    for peer in peers:
        pl.semaphore_signal(barrier, inc=1, device_id=peer, device_id_type=MESH)
    pl.semaphore_wait(barrier, len(peers))


class Sender:
    def __init__(self, send_sem, recv_sem):
        self.send_sem, self.recv_sem, self.count, self.open = send_sem, recv_sem, 0, []

    def start(self, src, dst, peer):
        copy = pltpu.make_async_remote_copy(
            src_ref=src,
            dst_ref=dst,
            send_sem=self.send_sem.at[self.count],
            recv_sem=self.recv_sem.at[self.count],
            device_id=peer,
            device_id_type=MESH,
        )
        copy.start()
        self.count += 1
        self.open.append(copy)
        return copy

    def drain(self):
        for copy in self.open:
            copy.wait_send()


def front_copies(seq_n, exp_n):
    half = exp_n // 2
    seq, rest = seq_n - 1, half - 1
    stats = 1 + seq + rest
    reduce = 1 + seq + rest + seq
    gather = seq + 2 * (rest + seq + 1)
    return stats + reduce + gather


def as_column(row, n):
    eye = lax.broadcasted_iota(jnp.int32, (n, n), 0) == lax.broadcasted_iota(jnp.int32, (n, n), 1)
    return jnp.sum(jnp.where(eye, jnp.broadcast_to(row, (n, n)), 0.0), axis=1, keepdims=True)


def as_row(column, n):
    eye = lax.broadcasted_iota(jnp.int32, (n, n), 0) == lax.broadcasted_iota(jnp.int32, (n, n), 1)
    return jnp.sum(jnp.where(eye, jnp.broadcast_to(column, (n, n)), 0.0), axis=0, keepdims=True)


def row_softmax(lg):
    q = jnp.exp(lg - jnp.max(lg, axis=1, keepdims=True))
    return q / jnp.sum(q, axis=1, keepdims=True)


def front(
    seq_n, exp_n, tok, rt, gout, win_hbm, wout_hbm,
    so_o, sg_o, st_o, x_o, g_o, hid_o, pg_o,
    win, wout, xt, qt, st_a, st_p, st_b, st_s, st_c, st_z,
    buf_a, rcv_a, buf_b, rcv_b, buf_c, rcv_c, xf, xg, buf_e, rcv_e, ag, inn, acc_p,
    w_sem, send_sem, recv_sem,
):
    clips, rows, width = tok.shape
    slots = rt.shape[1]
    half = exp_n // 2
    owned = slots // exp_n
    dc = width // seq_n
    kinds = 2 * clips
    experts = win.shape[0]
    s, h, par, pair, seq_peers, exp_peers = place(seq_n, exp_n)

    load_in = pltpu.make_async_copy(win_hbm, win, w_sem.at[0])
    load_out = pltpu.make_async_copy(wout_hbm, wout, w_sem.at[1])
    load_in.start()
    load_out.start()
    net = Sender(send_sem, recv_sem)

    peaks, masses = [], []
    for c in range(clips):
        lg = dot(tok[c], rt[...])
        m = jnp.max(lg, axis=0, keepdims=True)
        p = jnp.exp(lg - m)
        peaks.append(m)
        masses.append(jnp.sum(p, axis=0, keepdims=True))
        xt[c] = p.T.astype(BF16)
        qt[c] = row_softmax(lg).T.astype(BF16)
    pad = jnp.zeros((8 - 2 * clips, slots), F32)
    st_a[...] = jnp.concatenate(peaks + masses + [pad], axis=0)

    def combine(parts):
        m = parts[0][:clips]
        for part in parts[1:]:
            m = jnp.maximum(m, part[:clips])
        mass = None
        for part in parts:
            term = part[clips : 2 * clips] * jnp.exp(part[:clips] - m)
            mass = term if mass is None else mass + term
        return jnp.concatenate([m, mass, pad], axis=0)

    def lay_out(value, kind):
        for t in range(seq_n):
            block = value[:, t * dc : (t + 1) * dc].reshape(half, 2, owned, dc).astype(BF16)
            for q in range(2):
                buf_a[q, :, t, kind] = block[:, q]

    greet([pair] + seq_peers + exp_peers)
    copies = [net.start(st_a, st_p, pair)]
    lay_out(dot(qt[0], gout[0]), clips)
    copies[0].wait_recv()
    st_b[...] = combine([st_a[...], st_p[...]])
    copies = [net.start(st_b, st_s.at[k], peer) for k, peer in enumerate(seq_peers)]
    for c in range(1, clips):
        lay_out(dot(qt[c], gout[c]), clips + c)
    for copy in copies:
        copy.wait_recv()
    st_c[...] = combine([st_b[...]] + [st_s[k] for k in range(seq_n - 1)])
    copies = [net.start(st_c, st_z.at[k], peer) for k, peer in enumerate(exp_peers)]
    for c in range(clips):
        acc_p[c] = dot(xt[c], tok[c])
    for copy in copies:
        copy.wait_recv()
    stats = combine([st_c[...]] + [st_z[k] for k in range(half - 1)])
    scale = jnp.exp(st_a[:clips] - stats[:clips]) / stats[clips : 2 * clips]
    for c in range(clips):
        lay_out(acc_p[c] * as_column(scale[c : c + 1], slots), c)

    copy = net.start(buf_a.at[1 - par], rcv_a, pair)
    copy.wait_recv()
    for t in range(seq_n):
        buf_b[t] = (buf_a[par, :, t].astype(F32) + rcv_a[:, t].astype(F32)).astype(BF16)
    copies = [net.start(buf_b.at[peer[0]], rcv_b.at[k], peer) for k, peer in enumerate(seq_peers)]
    for copy in copies:
        copy.wait_recv()
    total = buf_b[s].astype(F32)
    for k in range(seq_n - 1):
        total = total + rcv_b[k].astype(F32)
    buf_c[...] = total.astype(BF16)
    copies = [
        net.start(buf_c.at[(h + 1 + k) % half], rcv_c.at[k], peer) for k, peer in enumerate(exp_peers)
    ]
    for copy in copies:
        copy.wait_recv()
    total = buf_c[h].astype(F32)
    for k in range(half - 1):
        total = total + rcv_c[k].astype(F32)
    xf[...] = total
    xg[s] = total.astype(BF16)
    copies = [net.start(xg.at[s], xg.at[s], peer) for peer in seq_peers]
    for copy in copies:
        copy.wait_recv()

    both = jnp.concatenate(
        [xg[t].astype(F32).reshape(kinds * owned, dc) for t in range(seq_n)], axis=1
    )
    n_rows = clips * owned
    x_rows, g_rows = both[:n_rows], both[n_rows:].astype(BF16)
    row = lax.broadcasted_iota(jnp.int32, (n_rows, 1), 0)
    expert_of = (row % owned) // (owned // experts)
    mask = [(expert_of == e).astype(F32) for e in range(experts)]
    load_in.wait()
    load_out.wait()
    pre, hidden_grad = 0.0, 0.0
    for e in range(experts):
        mine = x_rows * mask[e]
        x_o[e] = mine
        pre = pre + dot(mine.astype(BF16), win[e])
        hidden_grad = hidden_grad + dot_nt(g_rows, wout[e]) * mask[e]
    g_o[...] = g_rows
    hidden, back = jax.vjp(jax.nn.gelu, pre)
    pre_grad = back(hidden_grad)[0]
    pg_o[...] = pre_grad.astype(BF16)
    out_part, in_part = 0.0, 0.0
    for e in range(experts):
        mine = hidden * mask[e]
        hid_o[e] = mine
        out_part = out_part + dot(mine.astype(BF16), wout[e])
        in_part = in_part + dot_nt((pre_grad * mask[e]).astype(BF16), win[e])
    for t in range(seq_n):
        cut = slice(t * dc, (t + 1) * dc)
        buf_e[t, :clips] = out_part[:, cut].reshape(clips, owned, dc).astype(BF16)
        buf_e[t, clips:] = in_part[:, cut].reshape(clips, owned, dc).astype(BF16)
    copies = [net.start(buf_e.at[peer[0]], rcv_e.at[k], peer) for k, peer in enumerate(seq_peers)]
    for copy in copies:
        copy.wait_recv()
    total = buf_e[s].astype(F32)
    for k in range(seq_n - 1):
        total = total + rcv_e[k].astype(F32)
    piece = total.astype(BF16)
    ag[par, h, s] = piece
    inner = jnp.sum(piece[clips:].astype(F32) * xf[:clips], axis=2, keepdims=True)
    inn[par, h, s] = jnp.broadcast_to(inner, inn.shape[3:])

    copies = []
    for peer in exp_peers:
        copies.append(net.start(ag.at[par, h, s], ag.at[par, h, s], peer))
        copies.append(net.start(inn.at[par, h, s], inn.at[par, h, s], peer))
    for copy in copies:
        copy.wait_recv()
    copies = []
    for peer in seq_peers:
        copies.append(net.start(ag.at[par, :, s], ag.at[par, :, s], peer))
        copies.append(net.start(inn.at[par, :, s], inn.at[par, :, s], peer))
    for copy in copies:
        copy.wait_recv()
    copies = [net.start(ag.at[par], ag.at[par], pair), net.start(inn.at[par], inn.at[par], pair)]
    for copy in copies:
        copy.wait_recv()

    owners = [(q, g) for g in range(half) for q in range(2)]
    inners = []
    for c in range(clips):
        for t in range(seq_n):
            cut = slice(t * dc, (t + 1) * dc)
            for out, kind in ((so_o, c), (sg_o, clips + c)):
                out[c, :, cut] = jnp.concatenate(
                    [ag[q, g, t, kind].astype(F32) for q, g in owners], axis=0
                ).astype(BF16)
        parts = []
        for q, g in owners:
            part = inn[q, g, 0, c]
            for t in range(1, seq_n):
                part = part + inn[q, g, t, c]
            parts.append(part)
        inners.append(as_row(jnp.concatenate(parts, axis=0)[:, :1], slots))
    st_o[...] = jnp.concatenate([stats[: 2 * clips]] + inners + [jnp.zeros((8 - 3 * clips, slots), F32)], axis=0)
    net.drain()


def finish(clips, steps, tok, gout, rt, so, sg, st, x, g, hid, pg, mixed, gt, gr, gwin, gwout):
    i = pl.program_id(0)
    c = i // (steps // clips)
    peak = st[pl.ds(c, 1), :]
    mass = st[pl.ds(clips + c, 1), :]
    inner = st[pl.ds(2 * clips + c, 1), :]
    t, go = tok[0], gout[0]
    lg = dot(t, rt[...])
    dispatch = jnp.exp(lg - peak) / mass
    mixing = row_softmax(lg)
    mixing_grad = dot_nt(go, so[0])
    dispatch_grad = dot_nt(t, sg[0])
    lgrad = dispatch * (dispatch_grad - inner) + mixing * (
        mixing_grad - jnp.sum(mixing * mixing_grad, axis=1, keepdims=True)
    )
    mixed[0] = dot(mixing.astype(BF16), so[0]).astype(BF16)
    gt[0] = (dot(dispatch.astype(BF16), sg[0]) + dot_nt(lgrad.astype(BF16), rt[...])).astype(BF16)

    @pl.when(i == 0)
    def _():
        gr[...] = jnp.zeros_like(gr)

    gr[...] += dot(lgrad.T.astype(BF16), t)
    gwin[0] = dot(x[0].T.astype(BF16), pg[...]).astype(BF16)
    gwout[0] = dot(hid[0].T.astype(BF16), g[...]).astype(BF16)


def scatter(seq_n, exp_n, gr, out, buf_a, rcv_a, buf_b, rcv_b, buf_c, rcv_c, send_sem, recv_sem):
    half = exp_n // 2
    s, h, par, pair, seq_peers, exp_peers = place(seq_n, exp_n)
    rows = out.shape[0]
    net = Sender(send_sem, recv_sem)
    whole = gr[...].T
    for t in range(seq_n):
        for g in range(half):
            for q in range(2):
                at = (t * exp_n + 2 * g + q) * rows
                buf_a[q, t, g] = whole[at : at + rows]
    greet([pair] + seq_peers + exp_peers)
    net.start(buf_a.at[1 - par], rcv_a, pair).wait_recv()
    buf_b[...] = buf_a[par] + rcv_a[...]
    copies = [net.start(buf_b.at[peer[0]], rcv_b.at[k], peer) for k, peer in enumerate(seq_peers)]
    for copy in copies:
        copy.wait_recv()
    total = buf_b[s]
    for k in range(seq_n - 1):
        total = total + rcv_b[k]
    buf_c[...] = total
    copies = [
        net.start(buf_c.at[(h + 1 + k) % half], rcv_c.at[k], peer) for k, peer in enumerate(exp_peers)
    ]
    for copy in copies:
        copy.wait_recv()
    total = buf_c[h]
    for k in range(half - 1):
        total = total + rcv_c[k]
    out[...] = total
    net.drain()


def on_device(seq_n, exp_n, tokens, router, w_in, w_out, grad_out):
    clips, rows, width = tokens.shape
    slots = router.shape[1]
    experts, _, ff = w_in.shape
    half = exp_n // 2
    owned = slots // exp_n
    dc = width // seq_n
    kinds = 2 * clips
    n_rows = clips * owned
    vmem = pl.BlockSpec(memory_space=pltpu.VMEM)
    hbm = pl.BlockSpec(memory_space=pltpu.HBM)
    shape = jax.ShapeDtypeStruct
    block = (kinds, owned, dc)
    n_front = front_copies(seq_n, exp_n)
    so, sg, st, x, g, hid, pg = pl.pallas_call(
        functools.partial(front, seq_n, exp_n),
        out_shape=(
            shape((clips, slots, width), BF16),
            shape((clips, slots, width), BF16),
            shape((8, slots), F32),
            shape((experts, n_rows, width), F32),
            shape((n_rows, width), BF16),
            shape((experts, n_rows, ff), F32),
            shape((n_rows, ff), BF16),
        ),
        in_specs=[vmem, vmem, vmem, hbm, hbm],
        out_specs=(vmem,) * 7,
        scratch_shapes=[
            pltpu.VMEM(w_in.shape, BF16),
            pltpu.VMEM(w_out.shape, BF16),
            pltpu.VMEM((clips, slots, rows), BF16),
            pltpu.VMEM((clips, slots, rows), BF16),
            pltpu.VMEM((8, slots), F32),
            pltpu.VMEM((8, slots), F32),
            pltpu.VMEM((8, slots), F32),
            pltpu.VMEM((seq_n - 1, 8, slots), F32),
            pltpu.VMEM((8, slots), F32),
            pltpu.VMEM((half - 1, 8, slots), F32),
            pltpu.VMEM((2, half, seq_n) + block, BF16),
            pltpu.VMEM((half, seq_n) + block, BF16),
            pltpu.VMEM((seq_n, half) + block, BF16),
            pltpu.VMEM((seq_n - 1, half) + block, BF16),
            pltpu.VMEM((half,) + block, BF16),
            pltpu.VMEM((half - 1,) + block, BF16),
            pltpu.VMEM(block, F32),
            pltpu.VMEM((seq_n,) + block, BF16),
            pltpu.VMEM((seq_n,) + block, BF16),
            pltpu.VMEM((seq_n - 1,) + block, BF16),
            pltpu.VMEM((2, half, seq_n) + block, BF16),
            pltpu.VMEM((2, half, seq_n, clips, owned, 128), F32),
            pltpu.VMEM((clips, slots, width), F32),
            pltpu.SemaphoreType.DMA((2,)),
            pltpu.SemaphoreType.DMA((n_front,)),
            pltpu.SemaphoreType.DMA((n_front,)),
        ],
        compiler_params=pltpu.CompilerParams(collective_id=0, has_side_effects=True),
        name="front",
    )(tokens, router, grad_out, w_in, w_out)

    steps = 4 * clips
    t_blocks = steps // clips
    w_blocks = steps // experts
    token_spec = pl.BlockSpec((1, rows // t_blocks, width), lambda i: (i // t_blocks, i % t_blocks, 0))
    slot_spec = pl.BlockSpec((1, slots, width), lambda i: (i // t_blocks, 0, 0))

    def fixed(a):
        return pl.BlockSpec(a.shape, lambda i: (0,) * a.ndim)

    mixed, grad_tokens, gr, grad_w_in, grad_w_out = pl.pallas_call(
        functools.partial(finish, clips, steps),
        grid=(steps,),
        out_shape=(
            shape(tokens.shape, BF16),
            shape(tokens.shape, BF16),
            shape((slots, width), F32),
            shape(w_in.shape, BF16),
            shape(w_out.shape, BF16),
        ),
        in_specs=[
            token_spec,
            token_spec,
            fixed(router),
            slot_spec,
            slot_spec,
            fixed(st),
            pl.BlockSpec((1, n_rows, width // w_blocks), lambda i: (i // w_blocks, 0, i % w_blocks)),
            fixed(g),
            pl.BlockSpec((1, n_rows, ff // w_blocks), lambda i: (i // w_blocks, 0, i % w_blocks)),
            fixed(pg),
        ],
        out_specs=(
            token_spec,
            token_spec,
            pl.BlockSpec((slots, width), lambda i: (0, 0)),
            pl.BlockSpec((1, width // w_blocks, ff), lambda i: (i // w_blocks, i % w_blocks, 0)),
            pl.BlockSpec((1, ff // w_blocks, width), lambda i: (i // w_blocks, i % w_blocks, 0)),
        ),
        name="finish",
    )(tokens, grad_out, router, so, sg, st, x, g, hid, pg)

    out_rows = width // (seq_n * exp_n)
    n_scatter = 1 + (seq_n - 1) + (half - 1)
    tile = (out_rows, slots)
    grad_router = pl.pallas_call(
        functools.partial(scatter, seq_n, exp_n),
        out_shape=shape(tile, F32),
        in_specs=[vmem],
        out_specs=vmem,
        scratch_shapes=[
            pltpu.VMEM((2, seq_n, half) + tile, F32),
            pltpu.VMEM((seq_n, half) + tile, F32),
            pltpu.VMEM((seq_n, half) + tile, F32),
            pltpu.VMEM((seq_n - 1, half) + tile, F32),
            pltpu.VMEM((half,) + tile, F32),
            pltpu.VMEM((half - 1,) + tile, F32),
            pltpu.SemaphoreType.DMA((n_scatter,)),
            pltpu.SemaphoreType.DMA((n_scatter,)),
        ],
        compiler_params=pltpu.CompilerParams(collective_id=1, has_side_effects=True),
        name="scatter",
    )(gr)
    return mixed, grad_tokens, grad_router, grad_w_in, grad_w_out


def solution(mesh):
    return jax.shard_map(
        functools.partial(on_device, mesh.shape["seq"], mesh.shape["exp"]),
        mesh=mesh,
        in_specs=(
            P(None, ("seq", "exp"), None),
            P(),
            P("exp", None, "seq"),
            P("exp", "seq", None),
            P(None, ("seq", "exp"), None),
        ),
        out_specs=(
            P(None, ("seq", "exp"), None),
            P(None, ("seq", "exp"), None),
            P(("seq", "exp"), None),
            P("exp", None, "seq"),
            P("exp", "seq", None),
        ),
        check_vma=False,
    )
```

```python
import functools

import jax
import jax.numpy as jnp
from jax import lax
from jax.experimental import pallas as pl
from jax.experimental.pallas import tpu as pltpu
from jax.sharding import PartitionSpec as P

MESH = pl.DeviceIdType.MESH
F32 = jnp.float32
BF16 = jnp.bfloat16
NT = (((1,), (1,)), ((), ()))


def dot(a, b):
    return jnp.dot(a, b, preferred_element_type=F32)


def dot_nt(a, b):
    return lax.dot_general(a, b, NT, preferred_element_type=F32)


def place(seq_n, exp_n):
    s = lax.axis_index("seq")
    e = lax.axis_index("exp")
    h, par = e // 2, e % 2
    pair = (s, h * 2 + (1 - par))
    seq_peers = [((s + k) % seq_n, e) for k in range(1, seq_n)]
    exp_peers = [(s, ((h + k) % (exp_n // 2)) * 2 + par) for k in range(1, exp_n // 2)]
    return s, h, par, pair, seq_peers, exp_peers


def greet(peers):
    barrier = pltpu.get_barrier_semaphore()
    for peer in peers:
        pl.semaphore_signal(barrier, inc=1, device_id=peer, device_id_type=MESH)


def await_greetings(peers):
    pl.semaphore_wait(pltpu.get_barrier_semaphore(), len(peers))


class Sender:
    def __init__(self, send_sem, recv_sem):
        self.send_sem, self.recv_sem, self.count, self.open = send_sem, recv_sem, 0, []

    def start(self, src, dst, peer):
        copy = pltpu.make_async_remote_copy(
            src_ref=src,
            dst_ref=dst,
            send_sem=self.send_sem.at[self.count],
            recv_sem=self.recv_sem.at[self.count],
            device_id=peer,
            device_id_type=MESH,
        )
        copy.start()
        self.count += 1
        self.open.append(copy)
        return copy

    def drain(self):
        for copy in self.open:
            copy.wait_send()


def front_copies(seq_n, exp_n):
    seq, rest = seq_n - 1, exp_n // 2 - 1
    gather = 1 + seq + rest
    return gather + 2 * (gather + seq) + 2 * seq + 3 * gather


def as_column(row, n):
    eye = lax.broadcasted_iota(jnp.int32, (n, n), 0) == lax.broadcasted_iota(jnp.int32, (n, n), 1)
    return jnp.sum(jnp.where(eye, jnp.broadcast_to(row, (n, n)), 0.0), axis=1, keepdims=True)


def as_row(column, n):
    eye = lax.broadcasted_iota(jnp.int32, (n, n), 0) == lax.broadcasted_iota(jnp.int32, (n, n), 1)
    return jnp.sum(jnp.where(eye, jnp.broadcast_to(column, (n, n)), 0.0), axis=0, keepdims=True)


def row_softmax(lg):
    q = jnp.exp(lg - jnp.max(lg, axis=1, keepdims=True))
    return q / jnp.sum(q, axis=1, keepdims=True)


def front(
    seq_n, exp_n, tok_hbm, rt, gout_hbm, win_hbm, wout_hbm,
    so_o, wr_o, st_o, x_o, g_o, hid_o, pg_o,
    tok, gout, win, wout, xt, qt, st_a, st_p, st_b, st_s, st_c, st_z,
    buf_a, rcv_a, buf_b, rcv_b, buf_c, rcv_c, xf, xg, buf_e, rcv_e, ag, inn, acc_p,
    w_sem, send_sem, recv_sem,
):
    clips, rows, width = tok.shape
    slots = rt.shape[0]
    half = exp_n // 2
    owned = slots // exp_n
    dc = width // seq_n
    n_rows = clips * owned
    experts = win.shape[0]
    s, h, par, pair, seq_peers, exp_peers = place(seq_n, exp_n)

    load_tok = [pltpu.make_async_copy(tok_hbm.at[c], tok.at[c], w_sem.at[c]) for c in range(clips)]
    load_gout = [
        pltpu.make_async_copy(gout_hbm.at[c], gout.at[c], w_sem.at[clips + c]) for c in range(clips)
    ]
    load_in = pltpu.make_async_copy(win_hbm, win, w_sem.at[2 * clips])
    load_out = pltpu.make_async_copy(wout_hbm, wout, w_sem.at[2 * clips + 1])
    for load in load_tok + load_gout:
        load.start()
    greet([pair] + seq_peers + exp_peers)
    net = Sender(send_sem, recv_sem)

    peaks, masses = [], []
    for c in range(clips):
        load_tok[c].wait()
        if c == clips - 1:
            load_out.start()
            load_in.start()
        lg = dot_nt(tok[c], rt[...])
        m = jnp.max(lg, axis=0, keepdims=True)
        p = jnp.exp(lg - m)
        peaks.append(m)
        masses.append(jnp.sum(p, axis=0, keepdims=True))
        xt[c] = p.T.astype(BF16)
        qt[c] = row_softmax(lg).T.astype(BF16)
    pad = jnp.zeros((8 - 2 * clips, slots), F32)
    st_a[...] = jnp.concatenate(peaks + masses + [pad], axis=0)

    def combine(parts):
        m = parts[0][:clips]
        for part in parts[1:]:
            m = jnp.maximum(m, part[:clips])
        mass = None
        for part in parts:
            term = part[clips : 2 * clips] * jnp.exp(part[:clips] - m)
            mass = term if mass is None else mass + term
        return jnp.concatenate([m, mass, pad], axis=0)

    def lay_out(value, kind, c):
        for t in range(seq_n):
            block = value[:, t * dc : (t + 1) * dc].reshape(half, 2, owned, dc).astype(BF16)
            for q in range(2):
                buf_a[kind, q, :, t, c] = block[:, q]

    def arrived(copies):
        for copy in copies:
            copy.wait_recv()

    def total_of(own, parts, count):
        total = own.astype(F32)
        for k in range(count):
            total = total + parts[k].astype(F32)
        return total

    def to_pair(kind):
        return [net.start(buf_a.at[kind, 1 - par], rcv_a.at[kind], pair)]

    def to_seq(kind):
        for t in range(seq_n):
            mine = buf_a[kind, par, :, t].astype(F32)
            buf_b[kind, t] = (mine + rcv_a[kind, :, t].astype(F32)).astype(BF16)
        return [
            net.start(buf_b.at[kind, peer[0]], rcv_b.at[kind, k], peer)
            for k, peer in enumerate(seq_peers)
        ]

    def to_exp(kind):
        buf_c[kind] = total_of(buf_b[kind, s], rcv_b.at[kind], seq_n - 1).astype(BF16)
        return [
            net.start(buf_c.at[kind, (h + 1 + k) % half], rcv_c.at[kind, k], peer)
            for k, peer in enumerate(exp_peers)
        ]

    def to_group(kind):
        total = total_of(buf_c[kind, h], rcv_c.at[kind], half - 1)
        if kind == 0:
            xf[...] = total
        xg[kind, s] = total.astype(BF16)
        return [net.start(xg.at[kind, s], xg.at[kind, s], peer) for peer in seq_peers]

    def rows_of(kind):
        return jnp.concatenate(
            [xg[kind, t].astype(F32).reshape(n_rows, dc) for t in range(seq_n)], axis=1
        )

    await_greetings([pair] + seq_peers + exp_peers)
    stat = [net.start(st_a, st_p, pair)]
    load_gout[0].wait()
    lay_out(dot(qt[0], gout[0]), 1, 0)
    arrived(stat)
    st_b[...] = combine([st_a[...], st_p[...]])
    stat = [net.start(st_b, st_s.at[k], peer) for k, peer in enumerate(seq_peers)]
    for c in range(1, clips):
        load_gout[c].wait()
        lay_out(dot(qt[c], gout[c]), 1, c)
    grads = to_pair(1)
    arrived(stat)
    st_c[...] = combine([st_b[...]] + [st_s[k] for k in range(seq_n - 1)])
    stat = [net.start(st_c, st_z.at[k], peer) for k, peer in enumerate(exp_peers)]
    for c in range(clips):
        acc_p[c] = dot(xt[c], tok[c])
        if c == 0:
            arrived(grads)
            grads = to_seq(1)
    arrived(stat)
    stats = combine([st_c[...]] + [st_z[k] for k in range(half - 1)])
    scale = jnp.exp(st_a[:clips] - stats[:clips]) / stats[clips : 2 * clips]
    for c in range(clips):
        lay_out(acc_p[c] * as_column(scale[c : c + 1], slots), 0, c)
    inputs = to_pair(0)
    arrived(grads)
    grads = to_exp(1)
    arrived(inputs)
    inputs = to_seq(0)
    arrived(grads)
    grads = to_group(1)
    arrived(inputs)
    inputs = to_exp(0)
    arrived(grads)

    row = lax.broadcasted_iota(jnp.int32, (n_rows, 1), 0)
    expert_of = (row % owned) // (owned // experts)
    mask = [(expert_of == e).astype(F32) for e in range(experts)]
    g_rows = rows_of(1).astype(BF16)
    g_o[...] = g_rows
    load_out.wait()
    hidden_grad = 0.0
    for e in range(experts):
        hidden_grad = hidden_grad + dot_nt(g_rows, wout[e]) * mask[e]
    load_in.wait()

    arrived(inputs)
    inputs = to_group(0)
    arrived(inputs)
    x_rows = rows_of(0)
    pre = 0.0
    for e in range(experts):
        mine = x_rows * mask[e]
        x_o[e] = mine
        pre = pre + dot(mine.astype(BF16), win[e])
    hidden, back = jax.vjp(jax.nn.gelu, pre)
    pre_grad = back(hidden_grad)[0]

    def share(kind, part):
        for t in range(seq_n):
            cut = slice(t * dc, (t + 1) * dc)
            buf_e[kind, t] = part[:, cut].reshape(clips, owned, dc).astype(BF16)
        return [
            net.start(buf_e.at[kind, peer[0]], rcv_e.at[kind, k], peer)
            for k, peer in enumerate(seq_peers)
        ]

    in_part = 0.0
    for e in range(experts):
        in_part = in_part + dot_nt((pre_grad * mask[e]).astype(BF16), win[e])
    backward = share(1, in_part)
    out_part = 0.0
    for e in range(experts):
        mine = hidden * mask[e]
        hid_o[e] = mine
        out_part = out_part + dot(mine.astype(BF16), wout[e])
    forward = share(0, out_part)
    pg_o[...] = pre_grad.astype(BF16)

    def gather_exp(kind):
        piece = total_of(buf_e[kind, s], rcv_e.at[kind], seq_n - 1).astype(BF16)
        ag[kind, par, h, s] = piece
        copies = []
        if kind == 1:
            inner = jnp.sum(piece.astype(F32) * xf[...], axis=2, keepdims=True)
            lane = lax.broadcasted_iota(jnp.int32, inn.shape[3:], 1)
            tile = jnp.zeros(inn.shape[3:], F32)
            for c in range(clips):
                tile = jnp.where(lane == c, inner[c], tile)
            inn[par, h, s] = tile
            for peer in exp_peers:
                copies.append(net.start(inn.at[par, h, s], inn.at[par, h, s], peer))
        for peer in exp_peers:
            copies.append(net.start(ag.at[kind, par, h, s], ag.at[kind, par, h, s], peer))
        return copies

    def gather_seq(kind):
        copies = []
        for peer in seq_peers:
            if kind == 1:
                copies.append(net.start(inn.at[par, :, s], inn.at[par, :, s], peer))
            copies.append(net.start(ag.at[kind, par, :, s], ag.at[kind, par, :, s], peer))
        return copies

    def gather_pair(kind):
        copies = [net.start(ag.at[kind, par], ag.at[kind, par], pair)]
        if kind == 1:
            copies.append(net.start(inn.at[par], inn.at[par], pair))
        return copies

    owners = [(q, g) for g in range(half) for q in range(2)]

    def write_out(kind):
        for c in range(clips):
            for t in range(seq_n):
                cut = slice(t * dc, (t + 1) * dc)
                value = jnp.concatenate(
                    [ag[kind, q, g, t, c].astype(F32) for q, g in owners], axis=0
                ).astype(BF16)
                if kind == 0:
                    so_o[c, :, cut] = value
                else:
                    wr_o[c, slots:, cut] = value

    arrived(backward)
    backward = gather_exp(1)
    arrived(forward)
    forward = gather_exp(0)
    for c in range(clips):
        wr_o[c, :slots] = rt[...]
    arrived(backward)
    backward = gather_seq(1)
    arrived(forward)
    forward = gather_seq(0)
    arrived(backward)
    backward = gather_pair(1)
    arrived(forward)
    forward = gather_pair(0)
    arrived(backward)
    write_out(1)
    parts = []
    for q, g in owners:
        part = inn[q, g, 0]
        for t in range(1, seq_n):
            part = part + inn[q, g, t]
        parts.append(part)
    inners = jnp.concatenate(parts, axis=0)
    inners = [as_row(inners[:, c : c + 1], slots) for c in range(clips)]
    st_o[...] = jnp.concatenate(
        [stats[: 2 * clips]] + inners + [jnp.zeros((8 - 3 * clips, slots), F32)], axis=0
    )
    arrived(forward)
    write_out(0)
    net.drain()


def finish(clips, steps, tok, gout, so, wr, st, x, g, hid, pg, mixed, gt, gr, gwin, gwout):
    i = pl.program_id(0)
    c = i // (steps // clips)
    slots = so.shape[1]
    peak = st[pl.ds(c, 1), :]
    mass = st[pl.ds(clips + c, 1), :]
    inner = st[pl.ds(2 * clips + c, 1), :]
    t, go = tok[0], gout[0]
    both = dot_nt(t, wr[0])
    lg, dispatch_grad = both[:, :slots], both[:, slots:]
    mixing_grad = dot_nt(go, so[0])
    dispatch = jnp.exp(lg - peak) / mass
    mixing = row_softmax(lg)
    lgrad = dispatch * (dispatch_grad - inner) + mixing * (
        mixing_grad - jnp.sum(mixing * mixing_grad, axis=1, keepdims=True)
    )
    mixed[0] = dot(mixing.astype(BF16), so[0]).astype(BF16)
    gt[0] = dot(jnp.concatenate([lgrad, dispatch], axis=1).astype(BF16), wr[0]).astype(BF16)

    @pl.when(i == 0)
    def _():
        gr[...] = jnp.zeros_like(gr)

    gr[...] += dot(lgrad.T.astype(BF16), t)
    gwin[0] = dot(x[0].T.astype(BF16), pg[...]).astype(BF16)
    gwout[0] = dot(hid[0].T.astype(BF16), g[...]).astype(BF16)


def scatter(seq_n, exp_n, gr, out, buf_a, rcv_a, buf_b, rcv_b, buf_c, rcv_c, send_sem, recv_sem):
    half = exp_n // 2
    s, h, par, pair, seq_peers, exp_peers = place(seq_n, exp_n)
    rows, slots = out.shape
    packed = buf_c.shape[1]
    pack = rows // packed
    greet([pair] + seq_peers + exp_peers)
    net = Sender(send_sem, recv_sem)
    whole = gr[...].T
    for t in range(seq_n):
        for g in range(half):
            for q in range(2):
                at = (t * exp_n + 2 * g + q) * rows
                parts = [whole[at + j * packed : at + (j + 1) * packed] for j in range(pack)]
                buf_a[q, t, g] = jnp.concatenate(parts, axis=1).astype(BF16)
    await_greetings([pair] + seq_peers + exp_peers)
    net.start(buf_a.at[1 - par], rcv_a, pair).wait_recv()
    buf_b[...] = (buf_a[par].astype(F32) + rcv_a[...].astype(F32)).astype(BF16)
    copies = [net.start(buf_b.at[peer[0]], rcv_b.at[k], peer) for k, peer in enumerate(seq_peers)]
    for copy in copies:
        copy.wait_recv()
    total = buf_b[s].astype(F32)
    for k in range(seq_n - 1):
        total = total + rcv_b[k].astype(F32)
    buf_c[...] = total.astype(BF16)
    copies = [
        net.start(buf_c.at[(h + 1 + k) % half], rcv_c.at[k], peer) for k, peer in enumerate(exp_peers)
    ]
    for copy in copies:
        copy.wait_recv()
    total = buf_c[h].astype(F32)
    for k in range(half - 1):
        total = total + rcv_c[k].astype(F32)
    for j in range(pack):
        out[j * packed : (j + 1) * packed] = total[:, j * slots : (j + 1) * slots]
    net.drain()


def on_device(seq_n, exp_n, tokens, router, w_in, w_out, grad_out):
    clips, rows, width = tokens.shape
    slots = router.shape[1]
    experts, _, ff = w_in.shape
    half = exp_n // 2
    owned = slots // exp_n
    dc = width // seq_n
    n_rows = clips * owned
    router_t = router.T
    vmem = pl.BlockSpec(memory_space=pltpu.VMEM)
    hbm = pl.BlockSpec(memory_space=pltpu.HBM)
    shape = jax.ShapeDtypeStruct
    block = (clips, owned, dc)
    n_front = front_copies(seq_n, exp_n)
    so, wr, st, x, g, hid, pg = pl.pallas_call(
        functools.partial(front, seq_n, exp_n),
        out_shape=(
            shape((clips, slots, width), BF16),
            shape((clips, 2 * slots, width), BF16),
            shape((8, slots), F32),
            shape((experts, n_rows, width), F32),
            shape((n_rows, width), BF16),
            shape((experts, n_rows, ff), F32),
            shape((n_rows, ff), BF16),
        ),
        in_specs=[hbm, vmem, hbm, hbm, hbm],
        out_specs=(vmem,) * 7,
        scratch_shapes=[
            pltpu.VMEM(tokens.shape, BF16),
            pltpu.VMEM(tokens.shape, BF16),
            pltpu.VMEM(w_in.shape, BF16),
            pltpu.VMEM(w_out.shape, BF16),
            pltpu.VMEM((clips, slots, rows), BF16),
            pltpu.VMEM((clips, slots, rows), BF16),
            pltpu.VMEM((8, slots), F32),
            pltpu.VMEM((8, slots), F32),
            pltpu.VMEM((8, slots), F32),
            pltpu.VMEM((seq_n - 1, 8, slots), F32),
            pltpu.VMEM((8, slots), F32),
            pltpu.VMEM((half - 1, 8, slots), F32),
            pltpu.VMEM((2, 2, half, seq_n) + block, BF16),
            pltpu.VMEM((2, half, seq_n) + block, BF16),
            pltpu.VMEM((2, seq_n, half) + block, BF16),
            pltpu.VMEM((2, seq_n - 1, half) + block, BF16),
            pltpu.VMEM((2, half) + block, BF16),
            pltpu.VMEM((2, half - 1) + block, BF16),
            pltpu.VMEM(block, F32),
            pltpu.VMEM((2, seq_n) + block, BF16),
            pltpu.VMEM((2, seq_n) + block, BF16),
            pltpu.VMEM((2, seq_n - 1) + block, BF16),
            pltpu.VMEM((2, 2, half, seq_n) + block, BF16),
            pltpu.VMEM((2, half, seq_n, owned, 128), F32),
            pltpu.VMEM((clips, slots, width), F32),
            pltpu.SemaphoreType.DMA((2 * clips + 2,)),
            pltpu.SemaphoreType.DMA((n_front,)),
            pltpu.SemaphoreType.DMA((n_front,)),
        ],
        compiler_params=pltpu.CompilerParams(collective_id=0, has_side_effects=True),
        name="front",
    )(tokens, router_t, grad_out, w_in, w_out)

    steps = 4 * clips
    t_blocks = steps // clips
    w_blocks = steps // experts
    token_spec = pl.BlockSpec((1, rows // t_blocks, width), lambda i: (i // t_blocks, i % t_blocks, 0))

    def slot_spec(a):
        return pl.BlockSpec((1,) + a.shape[1:], lambda i: (i // t_blocks, 0, 0))

    def fixed(a):
        return pl.BlockSpec(a.shape, lambda i: (0,) * a.ndim)

    mixed, grad_tokens, gr, grad_w_in, grad_w_out = pl.pallas_call(
        functools.partial(finish, clips, steps),
        grid=(steps,),
        out_shape=(
            shape(tokens.shape, BF16),
            shape(tokens.shape, BF16),
            shape((slots, width), F32),
            shape(w_in.shape, BF16),
            shape(w_out.shape, BF16),
        ),
        in_specs=[
            token_spec,
            token_spec,
            slot_spec(so),
            slot_spec(wr),
            fixed(st),
            pl.BlockSpec((1, n_rows, width // w_blocks), lambda i: (i // w_blocks, 0, i % w_blocks)),
            fixed(g),
            pl.BlockSpec((1, n_rows, ff // w_blocks), lambda i: (i // w_blocks, 0, i % w_blocks)),
            fixed(pg),
        ],
        out_specs=(
            token_spec,
            token_spec,
            pl.BlockSpec((slots, width), lambda i: (0, 0)),
            pl.BlockSpec((1, width // w_blocks, ff), lambda i: (i // w_blocks, i % w_blocks, 0)),
            pl.BlockSpec((1, ff // w_blocks, width), lambda i: (i // w_blocks, i % w_blocks, 0)),
        ),
        name="finish",
    )(tokens, grad_out, so, wr, st, x, g, hid, pg)

    out_rows = width // (seq_n * exp_n)
    n_scatter = 1 + (seq_n - 1) + (half - 1)
    pack = max(1, 128 // slots)
    tile = (out_rows // pack, slots * pack)
    grad_router = pl.pallas_call(
        functools.partial(scatter, seq_n, exp_n),
        out_shape=shape((out_rows, slots), F32),
        in_specs=[vmem],
        out_specs=vmem,
        scratch_shapes=[
            pltpu.VMEM((2, seq_n, half) + tile, BF16),
            pltpu.VMEM((seq_n, half) + tile, BF16),
            pltpu.VMEM((seq_n, half) + tile, BF16),
            pltpu.VMEM((seq_n - 1, half) + tile, BF16),
            pltpu.VMEM((half,) + tile, BF16),
            pltpu.VMEM((half - 1,) + tile, BF16),
            pltpu.SemaphoreType.DMA((n_scatter,)),
            pltpu.SemaphoreType.DMA((n_scatter,)),
        ],
        compiler_params=pltpu.CompilerParams(collective_id=1, has_side_effects=True),
        name="scatter",
    )(gr)
    return mixed, grad_tokens, grad_router, grad_w_in, grad_w_out


def solution(mesh):
    return jax.shard_map(
        functools.partial(on_device, mesh.shape["seq"], mesh.shape["exp"]),
        mesh=mesh,
        in_specs=(
            P(None, ("seq", "exp"), None),
            P(),
            P("exp", None, "seq"),
            P("exp", "seq", None),
            P(None, ("seq", "exp"), None),
        ),
        out_specs=(
            P(None, ("seq", "exp"), None),
            P(None, ("seq", "exp"), None),
            P(("seq", "exp"), None),
            P("exp", None, "seq"),
            P("exp", "seq", None),
        ),
        check_vma=False,
    )
```

```python
import functools

import jax
import jax.numpy as jnp
from jax import lax
from jax.experimental import pallas as pl
from jax.experimental.pallas import tpu as pltpu
from jax.sharding import PartitionSpec as P

MESH = pl.DeviceIdType.MESH
F32 = jnp.float32
BF16 = jnp.bfloat16
NT = (((1,), (1,)), ((), ()))


def dot(a, b):
    return jnp.dot(a, b, preferred_element_type=F32)


def dot_nt(a, b):
    return lax.dot_general(a, b, NT, preferred_element_type=F32)


def place(seq_n, exp_n):
    s = lax.axis_index("seq")
    e = lax.axis_index("exp")
    h, par = e // 2, e % 2
    pair = (s, h * 2 + (1 - par))
    seq_peers = [((s + k) % seq_n, e) for k in range(1, seq_n)]
    exp_peers = [(s, ((h + k) % (exp_n // 2)) * 2 + par) for k in range(1, exp_n // 2)]
    return s, h, par, pair, seq_peers, exp_peers


def greet(peers):
    barrier = pltpu.get_barrier_semaphore()
    for peer in peers:
        pl.semaphore_signal(barrier, inc=1, device_id=peer, device_id_type=MESH)


def await_greetings(peers):
    pl.semaphore_wait(pltpu.get_barrier_semaphore(), len(peers))


class Sender:
    def __init__(self, send_sem, recv_sem):
        self.send_sem, self.recv_sem, self.count, self.open = send_sem, recv_sem, 0, []

    def start(self, src, dst, peer):
        copy = pltpu.make_async_remote_copy(
            src_ref=src,
            dst_ref=dst,
            send_sem=self.send_sem.at[self.count],
            recv_sem=self.recv_sem.at[self.count],
            device_id=peer,
            device_id_type=MESH,
        )
        copy.start()
        self.count += 1
        self.open.append(copy)
        return copy

    def drain(self):
        for copy in self.open:
            copy.wait_send()


def front_copies(seq_n, exp_n):
    half = exp_n // 2
    seq, rest = seq_n - 1, half - 1
    stats = 1 + seq + rest
    gather = rest + half * seq + seq_n
    return stats + 2 * (stats + seq) + 2 * seq + 3 * gather


def as_row(column, n):
    eye = lax.broadcasted_iota(jnp.int32, (n, n), 0) == lax.broadcasted_iota(jnp.int32, (n, n), 1)
    return jnp.sum(jnp.where(eye, jnp.broadcast_to(column, (n, n)), 0.0), axis=0, keepdims=True)


def row_softmax(lg):
    q = jnp.exp(lg - jnp.max(lg, axis=1, keepdims=True))
    return q / jnp.sum(q, axis=1, keepdims=True)


def front(
    seq_n, exp_n, tok_hbm, rt, gout_hbm, win_hbm, wout_hbm,
    so_o, wr_o, st_o, x_o, g_o, hid_o, pg_o,
    tok, gout, win, wout, xt, qt, st_a, st_p, st_b, st_s, st_c, st_z,
    buf_a, rcv_a, buf_b, rcv_b, buf_c, rcv_c, xf, xg, buf_e, rcv_e, ag, inn, fac_a, fac_b, fac_c,
    w_sem, send_sem, recv_sem,
):
    clips, rows, width = tok.shape
    slots = rt.shape[0]
    half = exp_n // 2
    owned = slots // exp_n
    dc = width // seq_n
    n_rows = clips * owned
    experts = win.shape[0]
    s, h, par, pair, seq_peers, exp_peers = place(seq_n, exp_n)

    load_tok = [pltpu.make_async_copy(tok_hbm.at[c], tok.at[c], w_sem.at[c]) for c in range(clips)]
    load_gout = [
        pltpu.make_async_copy(gout_hbm.at[c], gout.at[c], w_sem.at[clips + c]) for c in range(clips)
    ]
    load_in = pltpu.make_async_copy(win_hbm, win, w_sem.at[2 * clips])
    load_out = pltpu.make_async_copy(wout_hbm, wout, w_sem.at[2 * clips + 1])
    for load in load_tok + load_gout:
        load.start()
    greet([pair] + seq_peers + exp_peers)
    net = Sender(send_sem, recv_sem)

    peaks, masses = [], []
    for c in range(clips):
        load_tok[c].wait()
        if c == clips - 1:
            load_out.start()
            load_in.start()
        lg = dot_nt(tok[c], rt[...])
        m = jnp.max(lg, axis=0, keepdims=True)
        p = jnp.exp(lg - m)
        peaks.append(m)
        masses.append(jnp.sum(p, axis=0, keepdims=True))
        xt[c] = p.T.astype(BF16)
        qt[c] = row_softmax(lg).T.astype(BF16)
    pad = jnp.zeros((8 - 2 * clips, slots), F32)
    st_a[...] = jnp.concatenate(peaks + masses + [pad], axis=0)

    def combine(parts):
        m = parts[0][:clips]
        for part in parts[1:]:
            m = jnp.maximum(m, part[:clips])
        mass = None
        for part in parts:
            term = part[clips : 2 * clips] * jnp.exp(part[:clips] - m)
            mass = term if mass is None else mass + term
        return jnp.concatenate([m, mass, pad], axis=0)

    def lay_out(value, kind, c):
        for t in range(seq_n):
            block = value[:, t * dc : (t + 1) * dc].reshape(half, 2, owned, dc).astype(BF16)
            for q in range(2):
                buf_a[kind, q, :, t, c] = block[:, q]

    def arrived(copies):
        for copy in copies:
            copy.wait_recv()

    def total_of(own, parts, count):
        total = own.astype(F32)
        for k in range(count):
            total = total + parts[k].astype(F32)
        return total

    def to_pair(kind):
        return [net.start(buf_a.at[kind, 1 - par], rcv_a.at[kind], pair)]

    def factors(ref, tiles, joint, norm=None):
        terms = [jnp.exp(tile[:clips] - joint[:clips]) for tile in tiles]
        if norm is not None:
            terms = [term / norm for term in terms]
        spare = ref.shape[3] - clips * len(tiles)
        if spare:
            terms.append(jnp.zeros((spare, slots), F32))
        columns = jnp.concatenate(terms, axis=0).T.reshape(half, 2, owned, ref.shape[3])
        for q in range(2):
            ref[q] = columns[:, q]

    def to_seq(kind):
        if kind == 0:
            factors(fac_a, [st_a[...], st_p[...]], st_b[...])
            fac = fac_a[par]
        for t in range(seq_n):
            for c in range(clips):
                mine = buf_a[kind, par, :, t, c].astype(F32)
                other = rcv_a[kind, :, t, c].astype(F32)
                if kind == 0:
                    mine = mine * fac[:, :, c : c + 1]
                    other = other * fac[:, :, clips + c : clips + c + 1]
                buf_b[kind, t, :, c] = (mine + other).astype(BF16)
        return [
            net.start(buf_b.at[kind, peer[0]], rcv_b.at[kind, k], peer)
            for k, peer in enumerate(seq_peers)
        ]

    def to_exp(kind):
        if kind == 0:
            factors(fac_b, [st_b[...]] + [st_s[k] for k in range(seq_n - 1)], st_c[...])
            fac = fac_b[par]
        for c in range(clips):
            total = buf_b[kind, s, :, c].astype(F32)
            if kind == 0:
                total = total * fac[:, :, c : c + 1]
            for k in range(seq_n - 1):
                part = rcv_b[kind, k, :, c].astype(F32)
                if kind == 0:
                    at = (k + 1) * clips + c
                    part = part * fac[:, :, at : at + 1]
                total = total + part
            buf_c[kind, :, c] = total.astype(BF16)
        return [
            net.start(buf_c.at[kind, (h + 1 + k) % half], rcv_c.at[kind, k], peer)
            for k, peer in enumerate(exp_peers)
        ]

    def to_group(kind):
        if kind == 0:
            tiles = [st_c[...]] + [st_z[k] for k in range(half - 1)]
            factors(fac_c, tiles, stats, stats[clips : 2 * clips])
            fac = fac_c[par, h]
        for c in range(clips):
            total = buf_c[kind, h, c].astype(F32)
            if kind == 0:
                total = total * fac[:, c : c + 1]
            for k in range(half - 1):
                part = rcv_c[kind, k, c].astype(F32)
                if kind == 0:
                    at = (k + 1) * clips + c
                    part = part * fac[:, at : at + 1]
                total = total + part
            if kind == 0:
                xf[c] = total
            xg[kind, s, c] = total.astype(BF16)
        return [net.start(xg.at[kind, s], xg.at[kind, s], peer) for peer in seq_peers]

    def rows_of(kind):
        return jnp.concatenate(
            [xg[kind, t].astype(F32).reshape(n_rows, dc) for t in range(seq_n)], axis=1
        )

    await_greetings([pair] + seq_peers + exp_peers)
    stat = [net.start(st_a, st_p, pair)]
    for c in range(clips):
        lay_out(dot(xt[c], tok[c]), 0, c)
    inputs = to_pair(0)
    load_gout[0].wait()
    lay_out(dot(qt[0], gout[0]), 1, 0)
    arrived(stat)
    st_b[...] = combine([st_a[...], st_p[...]])
    stat = [net.start(st_b, st_s.at[k], peer) for k, peer in enumerate(seq_peers)]
    arrived(inputs)
    inputs = to_seq(0)
    for c in range(1, clips):
        load_gout[c].wait()
        lay_out(dot(qt[c], gout[c]), 1, c)
    grads = to_pair(1)
    arrived(stat)
    st_c[...] = combine([st_b[...]] + [st_s[k] for k in range(seq_n - 1)])
    stat = [net.start(st_c, st_z.at[k], peer) for k, peer in enumerate(exp_peers)]
    arrived(grads)
    grads = to_seq(1)
    arrived(inputs)
    inputs = to_exp(0)
    arrived(grads)
    grads = to_exp(1)
    arrived(stat)
    stats = combine([st_c[...]] + [st_z[k] for k in range(half - 1)])
    arrived(inputs)
    inputs = to_group(0)
    arrived(grads)
    grads = to_group(1)

    row = lax.broadcasted_iota(jnp.int32, (n_rows, 1), 0)
    expert_of = (row % owned) // (owned // experts)
    mask = [(expert_of == e).astype(F32) for e in range(experts)]
    load_out.wait()
    load_in.wait()
    arrived(inputs)
    x_rows = rows_of(0)
    pre = 0.0
    for e in range(experts):
        mine = x_rows * mask[e]
        x_o[e] = mine
        pre = pre + dot(mine.astype(BF16), win[e])
    arrived(grads)
    g_rows = rows_of(1).astype(BF16)
    g_o[...] = g_rows
    hidden_grad = 0.0
    for e in range(experts):
        hidden_grad = hidden_grad + dot_nt(g_rows, wout[e]) * mask[e]
    hidden, back = jax.vjp(jax.nn.gelu, pre)
    pre_grad = back(hidden_grad)[0]

    def share(kind, part):
        for t in range(seq_n):
            cut = slice(t * dc, (t + 1) * dc)
            buf_e[kind, t] = part[:, cut].reshape(clips, owned, dc).astype(BF16)
        return [
            net.start(buf_e.at[kind, peer[0]], rcv_e.at[kind, k], peer)
            for k, peer in enumerate(seq_peers)
        ]

    in_part = 0.0
    for e in range(experts):
        in_part = in_part + dot_nt((pre_grad * mask[e]).astype(BF16), win[e])
    backward = share(1, in_part)
    out_part = 0.0
    for e in range(experts):
        mine = hidden * mask[e]
        hid_o[e] = mine
        out_part = out_part + dot(mine.astype(BF16), wout[e])
    forward = share(0, out_part)
    pg_o[...] = pre_grad.astype(BF16)

    def send_piece(kind, peers, g, t):
        copies = []
        for peer in peers:
            at = ag.at[kind, par, g, t]
            copies.append([net.start(at, at, peer)])
            if kind == 1:
                at = inn.at[par, g, t]
                copies[-1].append(net.start(at, at, peer))
        return copies

    def send_column(kind, t):
        at = ag.at[kind, par, :, t]
        copies = [net.start(at, at, pair)]
        if kind == 1:
            at = inn.at[par, :, t]
            copies.append(net.start(at, at, pair))
        return copies

    def make_piece(kind):
        piece = total_of(buf_e[kind, s], rcv_e.at[kind], seq_n - 1).astype(BF16)
        ag[kind, par, h, s] = piece
        if kind == 1:
            inner = jnp.sum(piece.astype(F32) * xf[...], axis=2, keepdims=True)
            lane = lax.broadcasted_iota(jnp.int32, inn.shape[3:], 1)
            tile = jnp.zeros(inn.shape[3:], F32)
            for c in range(clips):
                tile = jnp.where(lane == c, inner[c], tile)
            inn[par, h, s] = tile
        along[kind] = send_piece(kind, exp_peers, h, s)
        across[kind] = [send_piece(kind, seq_peers, h, s)]

    owners = [(q, g) for g in range(half) for q in range(2)]

    def write_out(kind):
        for c in range(clips):
            for t in range(seq_n):
                cut = slice(t * dc, (t + 1) * dc)
                value = jnp.concatenate(
                    [ag[kind, q, g, t, c].astype(F32) for q, g in owners], axis=0
                ).astype(BF16)
                if kind == 0:
                    so_o[c, :, cut] = value
                else:
                    wr_o[c, slots:, cut] = value

    along, across, last = {}, {}, {}
    arrived(backward)
    make_piece(1)
    arrived(forward)
    make_piece(0)
    for c in range(clips):
        wr_o[c, :slots] = rt[...]
    for k in range(half - 1):
        source = (h + half - 1 - k) % half
        for kind in (1, 0):
            arrived(along[kind][k])
            across[kind].append(send_piece(kind, seq_peers, source, s))
    for kind in (1, 0):
        last[kind] = send_column(kind, s)
    for k in range(seq_n - 1):
        source = (s + seq_n - 1 - k) % seq_n
        for kind in (1, 0):
            for step in across[kind]:
                arrived(step[k])
            last[kind] += send_column(kind, source)
    backward, forward = last[1], last[0]
    arrived(backward)
    write_out(1)
    parts = []
    for q, g in owners:
        part = inn[q, g, 0]
        for t in range(1, seq_n):
            part = part + inn[q, g, t]
        parts.append(part)
    inners = jnp.concatenate(parts, axis=0)
    inners = [as_row(inners[:, c : c + 1], slots) for c in range(clips)]
    st_o[...] = jnp.concatenate(
        [stats[: 2 * clips]] + inners + [jnp.zeros((8 - 3 * clips, slots), F32)], axis=0
    )
    arrived(forward)
    write_out(0)
    net.drain()


def finish(clips, steps, tok, gout, so, wr, st, x, g, hid, pg, mixed, gt, gr, gwin, gwout):
    i = pl.program_id(0)
    c = i // (steps // clips)
    slots = so.shape[1]
    peak = st[pl.ds(c, 1), :]
    mass = st[pl.ds(clips + c, 1), :]
    inner = st[pl.ds(2 * clips + c, 1), :]
    t, go = tok[0], gout[0]
    both = dot_nt(t, wr[0])
    lg, dispatch_grad = both[:, :slots], both[:, slots:]
    mixing_grad = dot_nt(go, so[0])
    dispatch = jnp.exp(lg - peak) / mass
    mixing = row_softmax(lg)
    lgrad = dispatch * (dispatch_grad - inner) + mixing * (
        mixing_grad - jnp.sum(mixing * mixing_grad, axis=1, keepdims=True)
    )
    mixed[0] = dot(mixing.astype(BF16), so[0]).astype(BF16)
    gt[0] = dot(jnp.concatenate([lgrad, dispatch], axis=1).astype(BF16), wr[0]).astype(BF16)

    @pl.when(i == 0)
    def _():
        gr[...] = jnp.zeros_like(gr)

    gr[...] += dot(lgrad.T.astype(BF16), t)
    gwin[0] = dot(x[0].T.astype(BF16), pg[...]).astype(BF16)
    gwout[0] = dot(hid[0].T.astype(BF16), g[...]).astype(BF16)


def scatter(seq_n, exp_n, gr, out, buf_a, rcv_a, buf_b, rcv_b, send_sem, recv_sem):
    half = exp_n // 2
    s, h, par, pair, _, _ = place(seq_n, exp_n)
    ways = [(a, b) for a in range(seq_n) for b in range(half) if a or b]
    there = [((s + a) % seq_n, (h + b) % half) for a, b in ways]
    peers = [(t, g * 2 + par) for t, g in there]
    rows, slots = out.shape
    packed = buf_b.shape[2]
    pack = rows // packed
    greet([pair] + peers)
    net = Sender(send_sem, recv_sem)
    whole = gr[...].T
    for t in range(seq_n):
        for g in range(half):
            for q in range(2):
                at = (t * exp_n + 2 * g + q) * rows
                parts = [whole[at + j * packed : at + (j + 1) * packed] for j in range(pack)]
                buf_a[q, t, g] = jnp.concatenate(parts, axis=1).astype(BF16)
    await_greetings([pair] + peers)
    net.start(buf_a.at[1 - par], rcv_a, pair).wait_recv()
    buf_b[...] = (buf_a[par].astype(F32) + rcv_a[...].astype(F32)).astype(BF16)
    copies = [
        net.start(buf_b.at[t, g], rcv_b.at[k], peers[k]) for k, (t, g) in enumerate(there)
    ]
    total = buf_b[s, h].astype(F32)
    for k, copy in enumerate(copies):
        copy.wait_recv()
        total = total + rcv_b[k].astype(F32)
    for j in range(pack):
        out[j * packed : (j + 1) * packed] = total[:, j * slots : (j + 1) * slots]
    net.drain()


def on_device(seq_n, exp_n, tokens, router, w_in, w_out, grad_out):
    clips, rows, width = tokens.shape
    slots = router.shape[1]
    experts, _, ff = w_in.shape
    half = exp_n // 2
    owned = slots // exp_n
    dc = width // seq_n
    n_rows = clips * owned
    router_t = router.T
    vmem = pl.BlockSpec(memory_space=pltpu.VMEM)
    hbm = pl.BlockSpec(memory_space=pltpu.HBM)
    shape = jax.ShapeDtypeStruct
    block = (clips, owned, dc)
    n_front = front_copies(seq_n, exp_n)
    so, wr, st, x, g, hid, pg = pl.pallas_call(
        functools.partial(front, seq_n, exp_n),
        out_shape=(
            shape((clips, slots, width), BF16),
            shape((clips, 2 * slots, width), BF16),
            shape((8, slots), F32),
            shape((experts, n_rows, width), F32),
            shape((n_rows, width), BF16),
            shape((experts, n_rows, ff), F32),
            shape((n_rows, ff), BF16),
        ),
        in_specs=[hbm, vmem, hbm, hbm, hbm],
        out_specs=(vmem,) * 7,
        scratch_shapes=[
            pltpu.VMEM(tokens.shape, BF16),
            pltpu.VMEM(tokens.shape, BF16),
            pltpu.VMEM(w_in.shape, BF16),
            pltpu.VMEM(w_out.shape, BF16),
            pltpu.VMEM((clips, slots, rows), BF16),
            pltpu.VMEM((clips, slots, rows), BF16),
            pltpu.VMEM((8, slots), F32),
            pltpu.VMEM((8, slots), F32),
            pltpu.VMEM((8, slots), F32),
            pltpu.VMEM((seq_n - 1, 8, slots), F32),
            pltpu.VMEM((8, slots), F32),
            pltpu.VMEM((half - 1, 8, slots), F32),
            pltpu.VMEM((2, 2, half, seq_n) + block, BF16),
            pltpu.VMEM((2, half, seq_n) + block, BF16),
            pltpu.VMEM((2, seq_n, half) + block, BF16),
            pltpu.VMEM((2, seq_n - 1, half) + block, BF16),
            pltpu.VMEM((2, half) + block, BF16),
            pltpu.VMEM((2, half - 1) + block, BF16),
            pltpu.VMEM(block, F32),
            pltpu.VMEM((2, seq_n) + block, BF16),
            pltpu.VMEM((2, seq_n) + block, BF16),
            pltpu.VMEM((2, seq_n - 1) + block, BF16),
            pltpu.VMEM((2, 2, half, seq_n) + block, BF16),
            pltpu.VMEM((2, half, seq_n, owned, 128), F32),
            pltpu.VMEM((2, half, owned, -(-2 * clips // 8) * 8), F32),
            pltpu.VMEM((2, half, owned, -(-seq_n * clips // 8) * 8), F32),
            pltpu.VMEM((2, half, owned, -(-half * clips // 8) * 8), F32),
            pltpu.SemaphoreType.DMA((2 * clips + 2,)),
            pltpu.SemaphoreType.DMA((n_front,)),
            pltpu.SemaphoreType.DMA((n_front,)),
        ],
        compiler_params=pltpu.CompilerParams(collective_id=0, has_side_effects=True),
        name="front",
    )(tokens, router_t, grad_out, w_in, w_out)

    steps = 4 * clips
    t_blocks = steps // clips
    w_blocks = steps // experts
    token_spec = pl.BlockSpec((1, rows // t_blocks, width), lambda i: (i // t_blocks, i % t_blocks, 0))

    def slot_spec(a):
        return pl.BlockSpec((1,) + a.shape[1:], lambda i: (i // t_blocks, 0, 0))

    def fixed(a):
        return pl.BlockSpec(a.shape, lambda i: (0,) * a.ndim)

    mixed, grad_tokens, gr, grad_w_in, grad_w_out = pl.pallas_call(
        functools.partial(finish, clips, steps),
        grid=(steps,),
        out_shape=(
            shape(tokens.shape, BF16),
            shape(tokens.shape, BF16),
            shape((slots, width), F32),
            shape(w_in.shape, BF16),
            shape(w_out.shape, BF16),
        ),
        in_specs=[
            token_spec,
            token_spec,
            slot_spec(so),
            slot_spec(wr),
            fixed(st),
            pl.BlockSpec((1, n_rows, width // w_blocks), lambda i: (i // w_blocks, 0, i % w_blocks)),
            fixed(g),
            pl.BlockSpec((1, n_rows, ff // w_blocks), lambda i: (i // w_blocks, 0, i % w_blocks)),
            fixed(pg),
        ],
        out_specs=(
            token_spec,
            token_spec,
            pl.BlockSpec((slots, width), lambda i: (0, 0)),
            pl.BlockSpec((1, width // w_blocks, ff), lambda i: (i // w_blocks, i % w_blocks, 0)),
            pl.BlockSpec((1, ff // w_blocks, width), lambda i: (i // w_blocks, i % w_blocks, 0)),
        ),
        name="finish",
    )(tokens, grad_out, so, wr, st, x, g, hid, pg)

    out_rows = width // (seq_n * exp_n)
    n_scatter = seq_n * half
    pack = max(1, 128 // slots)
    tile = (out_rows // pack, slots * pack)
    grad_router = pl.pallas_call(
        functools.partial(scatter, seq_n, exp_n),
        out_shape=shape((out_rows, slots), F32),
        in_specs=[vmem],
        out_specs=vmem,
        scratch_shapes=[
            pltpu.VMEM((2, seq_n, half) + tile, BF16),
            pltpu.VMEM((seq_n, half) + tile, BF16),
            pltpu.VMEM((seq_n, half) + tile, BF16),
            pltpu.VMEM((seq_n * half - 1,) + tile, BF16),
            pltpu.SemaphoreType.DMA((n_scatter,)),
            pltpu.SemaphoreType.DMA((n_scatter,)),
        ],
        compiler_params=pltpu.CompilerParams(collective_id=1, has_side_effects=True),
        name="scatter",
    )(gr)
    return mixed, grad_tokens, grad_router, grad_w_in, grad_w_out


def solution(mesh):
    return jax.shard_map(
        functools.partial(on_device, mesh.shape["seq"], mesh.shape["exp"]),
        mesh=mesh,
        in_specs=(
            P(None, ("seq", "exp"), None),
            P(),
            P("exp", None, "seq"),
            P("exp", "seq", None),
            P(None, ("seq", "exp"), None),
        ),
        out_specs=(
            P(None, ("seq", "exp"), None),
            P(None, ("seq", "exp"), None),
            P(("seq", "exp"), None),
            P("exp", None, "seq"),
            P("exp", "seq", None),
        ),
        check_vma=False,
    )
```

```python
import functools

import jax
import jax.numpy as jnp
from jax import lax
from jax.experimental import pallas as pl
from jax.experimental.pallas import tpu as pltpu
from jax.sharding import PartitionSpec as P

MESH = pl.DeviceIdType.MESH
F32 = jnp.float32
BF16 = jnp.bfloat16
NT = (((1,), (1,)), ((), ()))


def dot(a, b):
    return jnp.dot(a, b, preferred_element_type=F32)


def dot_nt(a, b):
    return lax.dot_general(a, b, NT, preferred_element_type=F32)


def place(seq_n, exp_n):
    s = lax.axis_index("seq")
    e = lax.axis_index("exp")
    h, par = e // 2, e % 2
    pair = (s, h * 2 + (1 - par))
    seq_peers = [((s + k) % seq_n, e) for k in range(1, seq_n)]
    exp_peers = [(s, ((h + k) % (exp_n // 2)) * 2 + par) for k in range(1, exp_n // 2)]
    return s, h, par, pair, seq_peers, exp_peers


def greet(peers):
    barrier = pltpu.get_barrier_semaphore()
    for peer in peers:
        pl.semaphore_signal(barrier, inc=1, device_id=peer, device_id_type=MESH)


def await_greetings(peers):
    pl.semaphore_wait(pltpu.get_barrier_semaphore(), len(peers))


class Sender:
    def __init__(self, send_sem, recv_sem):
        self.send_sem, self.recv_sem, self.count, self.open = send_sem, recv_sem, 0, []

    def start(self, src, dst, peer):
        copy = pltpu.make_async_remote_copy(
            src_ref=src,
            dst_ref=dst,
            send_sem=self.send_sem.at[self.count],
            recv_sem=self.recv_sem.at[self.count],
            device_id=peer,
            device_id_type=MESH,
        )
        copy.start()
        self.count += 1
        self.open.append(copy)
        return copy

    def drain(self):
        for copy in self.open:
            copy.wait_send()


def front_copies(seq_n, exp_n):
    half = exp_n // 2
    seq, rest = seq_n - 1, half - 1
    stats = 1 + seq + rest
    gather = rest + half * seq + seq_n
    return stats + 2 * (stats + seq) + 2 * seq + 3 * gather


def as_row(column, n):
    eye = lax.broadcasted_iota(jnp.int32, (n, n), 0) == lax.broadcasted_iota(jnp.int32, (n, n), 1)
    return jnp.sum(jnp.where(eye, jnp.broadcast_to(column, (n, n)), 0.0), axis=0, keepdims=True)


def row_softmax(lg):
    q = jnp.exp(lg - jnp.max(lg, axis=1, keepdims=True))
    return q / jnp.sum(q, axis=1, keepdims=True)


def front(
    seq_n, exp_n, tok_hbm, rt, gout_hbm, win_hbm, wout_hbm,
    so_o, wr_o, st_o, x_o, g_o, hid_o, pg_o,
    tok, gout, win, wout, xt, qt, st_a, st_p, st_b, st_s, st_c, st_z,
    buf_a, rcv_a, buf_b, rcv_b, buf_c, rcv_c, xf, xg, buf_e, rcv_e, ag, inn, fac_a, fac_b, fac_c,
    w_sem, send_sem, recv_sem,
):
    clips, rows, width = tok.shape
    slots = rt.shape[0]
    half = exp_n // 2
    owned = slots // exp_n
    dc = width // seq_n
    n_rows = clips * owned
    experts = win.shape[0]
    s, h, par, pair, seq_peers, exp_peers = place(seq_n, exp_n)

    load_tok = [pltpu.make_async_copy(tok_hbm.at[c], tok.at[c], w_sem.at[c]) for c in range(clips)]
    load_gout = [
        pltpu.make_async_copy(gout_hbm.at[c], gout.at[c], w_sem.at[clips + c]) for c in range(clips)
    ]
    load_in = pltpu.make_async_copy(win_hbm, win, w_sem.at[2 * clips])
    load_out = pltpu.make_async_copy(wout_hbm, wout, w_sem.at[2 * clips + 1])
    for load in load_tok + load_gout:
        load.start()
    greet([pair] + seq_peers + exp_peers)
    net = Sender(send_sem, recv_sem)

    peaks, masses = [], []
    for c in range(clips):
        load_tok[c].wait()
        lg = dot_nt(tok[c], rt[...])
        m = jnp.max(lg, axis=0, keepdims=True)
        p = jnp.exp(lg - m)
        peaks.append(m)
        masses.append(jnp.sum(p, axis=0, keepdims=True))
        xt[c] = p.T.astype(BF16)
        qt[c] = row_softmax(lg).T.astype(BF16)
    pad = jnp.zeros((8 - 2 * clips, slots), F32)
    st_a[...] = jnp.concatenate(peaks + masses + [pad], axis=0)

    def combine(parts):
        m = parts[0][:clips]
        for part in parts[1:]:
            m = jnp.maximum(m, part[:clips])
        mass = None
        for part in parts:
            term = part[clips : 2 * clips] * jnp.exp(part[:clips] - m)
            mass = term if mass is None else mass + term
        return jnp.concatenate([m, mass, pad], axis=0)

    def lay_out(value, kind, c):
        for t in range(seq_n):
            block = value[:, t * dc : (t + 1) * dc].reshape(half, 2, owned, dc).astype(BF16)
            for q in range(2):
                buf_a[kind, q, :, t, c] = block[:, q]

    def arrived(copies):
        for copy in copies:
            copy.wait_recv()

    def total_of(own, parts, count):
        total = own.astype(F32)
        for k in range(count):
            total = total + parts[k].astype(F32)
        return total

    def to_pair(kind):
        return [net.start(buf_a.at[kind, 1 - par], rcv_a.at[kind], pair)]

    def factors(ref, tiles, joint, norm=None):
        terms = [jnp.exp(tile[:clips] - joint[:clips]) for tile in tiles]
        if norm is not None:
            terms = [term / norm for term in terms]
        spare = ref.shape[3] - clips * len(tiles)
        if spare:
            terms.append(jnp.zeros((spare, slots), F32))
        columns = jnp.concatenate(terms, axis=0).T.reshape(half, 2, owned, ref.shape[3])
        for q in range(2):
            ref[q] = columns[:, q]

    def to_seq(kind):
        if kind == 0:
            factors(fac_a, [st_a[...], st_p[...]], st_b[...])
            fac = fac_a[par]
        for t in range(seq_n):
            for c in range(clips):
                mine = buf_a[kind, par, :, t, c].astype(F32)
                other = rcv_a[kind, :, t, c].astype(F32)
                if kind == 0:
                    mine = mine * fac[:, :, c : c + 1]
                    other = other * fac[:, :, clips + c : clips + c + 1]
                buf_b[kind, t, :, c] = (mine + other).astype(BF16)
        return [
            net.start(buf_b.at[kind, peer[0]], rcv_b.at[kind, k], peer)
            for k, peer in enumerate(seq_peers)
        ]

    def to_exp(kind):
        if kind == 0:
            factors(fac_b, [st_b[...]] + [st_s[k] for k in range(seq_n - 1)], st_c[...])
            fac = fac_b[par]
        for c in range(clips):
            total = buf_b[kind, s, :, c].astype(F32)
            if kind == 0:
                total = total * fac[:, :, c : c + 1]
            for k in range(seq_n - 1):
                part = rcv_b[kind, k, :, c].astype(F32)
                if kind == 0:
                    at = (k + 1) * clips + c
                    part = part * fac[:, :, at : at + 1]
                total = total + part
            buf_c[kind, :, c] = total.astype(BF16)
        return [
            net.start(buf_c.at[kind, (h + 1 + k) % half], rcv_c.at[kind, k], peer)
            for k, peer in enumerate(exp_peers)
        ]

    def to_group(kind):
        if kind == 0:
            tiles = [st_c[...]] + [st_z[k] for k in range(half - 1)]
            factors(fac_c, tiles, stats, stats[clips : 2 * clips])
            fac = fac_c[par, h]
        for c in range(clips):
            total = buf_c[kind, h, c].astype(F32)
            if kind == 0:
                total = total * fac[:, c : c + 1]
            for k in range(half - 1):
                part = rcv_c[kind, k, c].astype(F32)
                if kind == 0:
                    at = (k + 1) * clips + c
                    part = part * fac[:, at : at + 1]
                total = total + part
            if kind == 0:
                xf[c] = total
            xg[kind, s, c] = total.astype(BF16)
        return [net.start(xg.at[kind, s], xg.at[kind, s], peer) for peer in seq_peers]

    def rows_of(kind):
        return jnp.concatenate(
            [xg[kind, t].astype(F32).reshape(n_rows, dc) for t in range(seq_n)], axis=1
        )

    await_greetings([pair] + seq_peers + exp_peers)
    stat = [net.start(st_a, st_p, pair)]
    for c in range(clips):
        lay_out(dot(xt[c], tok[c]), 0, c)
    inputs = to_pair(0)
    load_gout[0].wait()
    lay_out(dot(qt[0], gout[0]), 1, 0)
    arrived(stat)
    st_b[...] = combine([st_a[...], st_p[...]])
    stat = [net.start(st_b, st_s.at[k], peer) for k, peer in enumerate(seq_peers)]
    arrived(inputs)
    inputs = to_seq(0)
    for c in range(1, clips):
        load_gout[c].wait()
        lay_out(dot(qt[c], gout[c]), 1, c)
    load_in.start()
    load_out.start()
    grads = to_pair(1)
    arrived(stat)
    st_c[...] = combine([st_b[...]] + [st_s[k] for k in range(seq_n - 1)])
    stat = [net.start(st_c, st_z.at[k], peer) for k, peer in enumerate(exp_peers)]
    arrived(grads)
    grads = to_seq(1)
    arrived(inputs)
    inputs = to_exp(0)
    arrived(grads)
    grads = to_exp(1)
    arrived(stat)
    stats = combine([st_c[...]] + [st_z[k] for k in range(half - 1)])
    arrived(inputs)
    inputs = to_group(0)
    arrived(grads)
    grads = to_group(1)

    row = lax.broadcasted_iota(jnp.int32, (n_rows, 1), 0)
    expert_of = (row % owned) // (owned // experts)
    mask = [(expert_of == e).astype(F32) for e in range(experts)]
    load_in.wait()
    load_out.wait()
    arrived(inputs)
    x_rows = rows_of(0)
    pre = 0.0
    for e in range(experts):
        mine = x_rows * mask[e]
        x_o[e] = mine
        pre = pre + dot(mine.astype(BF16), win[e])
    hidden, back = jax.vjp(jax.nn.gelu, pre)

    def share(kind, part):
        for t in range(seq_n):
            cut = slice(t * dc, (t + 1) * dc)
            buf_e[kind, t] = part[:, cut].reshape(clips, owned, dc).astype(BF16)
        return [
            net.start(buf_e.at[kind, peer[0]], rcv_e.at[kind, k], peer)
            for k, peer in enumerate(seq_peers)
        ]

    out_part = 0.0
    for e in range(experts):
        mine = hidden * mask[e]
        hid_o[e] = mine
        out_part = out_part + dot(mine.astype(BF16), wout[e])
    forward = share(0, out_part)

    def send_piece(kind, peers, g, t):
        copies = []
        for peer in peers:
            at = ag.at[kind, par, g, t]
            copies.append([net.start(at, at, peer)])
            if kind == 1:
                at = inn.at[par, g, t]
                copies[-1].append(net.start(at, at, peer))
        return copies

    def send_column(kind, t):
        at = ag.at[kind, par, :, t]
        copies = [net.start(at, at, pair)]
        if kind == 1:
            at = inn.at[par, :, t]
            copies.append(net.start(at, at, pair))
        return copies

    def make_piece(kind):
        piece = total_of(buf_e[kind, s], rcv_e.at[kind], seq_n - 1).astype(BF16)
        ag[kind, par, h, s] = piece
        if kind == 1:
            inner = jnp.sum(piece.astype(F32) * xf[...], axis=2, keepdims=True)
            lane = lax.broadcasted_iota(jnp.int32, inn.shape[3:], 1)
            tile = jnp.zeros(inn.shape[3:], F32)
            for c in range(clips):
                tile = jnp.where(lane == c, inner[c], tile)
            inn[par, h, s] = tile
        along[kind] = send_piece(kind, exp_peers, h, s)
        across[kind] = [send_piece(kind, seq_peers, h, s)]

    owners = [(q, g) for g in range(half) for q in range(2)]

    def write_out(kind):
        for c in range(clips):
            for t in range(seq_n):
                cut = slice(t * dc, (t + 1) * dc)
                value = jnp.concatenate(
                    [ag[kind, q, g, t, c].astype(F32) for q, g in owners], axis=0
                ).astype(BF16)
                if kind == 0:
                    so_o[c, :, cut] = value
                else:
                    wr_o[c, slots:, cut] = value

    along, across, last = {}, {}, {}
    arrived(grads)
    g_rows = rows_of(1).astype(BF16)
    g_o[...] = g_rows
    hidden_grad = 0.0
    for e in range(experts):
        hidden_grad = hidden_grad + dot_nt(g_rows, wout[e]) * mask[e]
    arrived(forward)
    make_piece(0)
    pre_grad = back(hidden_grad)[0]
    in_part = 0.0
    for e in range(experts):
        in_part = in_part + dot_nt((pre_grad * mask[e]).astype(BF16), win[e])
    backward = share(1, in_part)
    pg_o[...] = pre_grad.astype(BF16)
    for c in range(clips):
        wr_o[c, :slots] = rt[...]
    for k in range(half - 1):
        arrived(along[0][k])
        across[0].append(send_piece(0, seq_peers, (h + half - 1 - k) % half, s))
    arrived(backward)
    make_piece(1)
    for k in range(half - 1):
        arrived(along[1][k])
        across[1].append(send_piece(1, seq_peers, (h + half - 1 - k) % half, s))
    for kind in (0, 1):
        last[kind] = send_column(kind, s)
    for k in range(seq_n - 1):
        source = (s + seq_n - 1 - k) % seq_n
        for kind in (0, 1):
            for step in across[kind]:
                arrived(step[k])
            last[kind] += send_column(kind, source)
    backward, forward = last[1], last[0]
    arrived(forward)
    write_out(0)
    arrived(backward)
    write_out(1)
    parts = []
    for q, g in owners:
        part = inn[q, g, 0]
        for t in range(1, seq_n):
            part = part + inn[q, g, t]
        parts.append(part)
    inners = jnp.concatenate(parts, axis=0)
    inners = [as_row(inners[:, c : c + 1], slots) for c in range(clips)]
    st_o[...] = jnp.concatenate(
        [stats[: 2 * clips]] + inners + [jnp.zeros((8 - 3 * clips, slots), F32)], axis=0
    )
    net.drain()


def finish(clips, steps, tok, gout, so, wr, st, x, g, hid, pg, mixed, gt, gr, gwin, gwout):
    i = pl.program_id(0)
    c = i // (steps // clips)
    slots = so.shape[1]
    peak = st[pl.ds(c, 1), :]
    mass = st[pl.ds(clips + c, 1), :]
    inner = st[pl.ds(2 * clips + c, 1), :]
    t, go = tok[0], gout[0]
    both = dot_nt(t, wr[0])
    lg, dispatch_grad = both[:, :slots], both[:, slots:]
    mixing_grad = dot_nt(go, so[0])
    dispatch = jnp.exp(lg - peak) / mass
    mixing = row_softmax(lg)
    lgrad = dispatch * (dispatch_grad - inner) + mixing * (
        mixing_grad - jnp.sum(mixing * mixing_grad, axis=1, keepdims=True)
    )
    mixed[0] = dot(mixing.astype(BF16), so[0]).astype(BF16)
    gt[0] = dot(jnp.concatenate([lgrad, dispatch], axis=1).astype(BF16), wr[0]).astype(BF16)

    @pl.when(i == 0)
    def _():
        gr[...] = jnp.zeros_like(gr)

    gr[...] += dot(lgrad.T.astype(BF16), t)
    gwin[0] = dot(x[0].T.astype(BF16), pg[...]).astype(BF16)
    gwout[0] = dot(hid[0].T.astype(BF16), g[...]).astype(BF16)


def scatter(seq_n, exp_n, gr, out, buf_a, rcv_a, buf_b, rcv_b, send_sem, recv_sem):
    half = exp_n // 2
    s, h, par, pair, _, _ = place(seq_n, exp_n)
    ways = [(a, b) for a in range(seq_n) for b in range(half) if a or b]
    there = [((s + a) % seq_n, (h + b) % half) for a, b in ways]
    peers = [(t, g * 2 + par) for t, g in there]
    rows, slots = out.shape
    packed = buf_b.shape[2]
    pack = rows // packed
    greet([pair] + peers)
    net = Sender(send_sem, recv_sem)
    whole = gr[...].T
    for t in range(seq_n):
        for g in range(half):
            for q in range(2):
                at = (t * exp_n + 2 * g + q) * rows
                parts = [whole[at + j * packed : at + (j + 1) * packed] for j in range(pack)]
                buf_a[q, t, g] = jnp.concatenate(parts, axis=1).astype(BF16)
    await_greetings([pair] + peers)
    net.start(buf_a.at[1 - par], rcv_a, pair).wait_recv()
    buf_b[...] = (buf_a[par].astype(F32) + rcv_a[...].astype(F32)).astype(BF16)
    copies = [
        net.start(buf_b.at[t, g], rcv_b.at[k], peers[k]) for k, (t, g) in enumerate(there)
    ]
    total = buf_b[s, h].astype(F32)
    for k, copy in enumerate(copies):
        copy.wait_recv()
        total = total + rcv_b[k].astype(F32)
    for j in range(pack):
        out[j * packed : (j + 1) * packed] = total[:, j * slots : (j + 1) * slots]
    net.drain()


def on_device(seq_n, exp_n, tokens, router, w_in, w_out, grad_out):
    clips, rows, width = tokens.shape
    slots = router.shape[1]
    experts, _, ff = w_in.shape
    half = exp_n // 2
    owned = slots // exp_n
    dc = width // seq_n
    n_rows = clips * owned
    router_t = router.T
    vmem = pl.BlockSpec(memory_space=pltpu.VMEM)
    hbm = pl.BlockSpec(memory_space=pltpu.HBM)
    shape = jax.ShapeDtypeStruct
    block = (clips, owned, dc)
    n_front = front_copies(seq_n, exp_n)
    so, wr, st, x, g, hid, pg = pl.pallas_call(
        functools.partial(front, seq_n, exp_n),
        out_shape=(
            shape((clips, slots, width), BF16),
            shape((clips, 2 * slots, width), BF16),
            shape((8, slots), F32),
            shape((experts, n_rows, width), F32),
            shape((n_rows, width), BF16),
            shape((experts, n_rows, ff), F32),
            shape((n_rows, ff), BF16),
        ),
        in_specs=[hbm, vmem, hbm, hbm, hbm],
        out_specs=(vmem,) * 7,
        scratch_shapes=[
            pltpu.VMEM(tokens.shape, BF16),
            pltpu.VMEM(tokens.shape, BF16),
            pltpu.VMEM(w_in.shape, BF16),
            pltpu.VMEM(w_out.shape, BF16),
            pltpu.VMEM((clips, slots, rows), BF16),
            pltpu.VMEM((clips, slots, rows), BF16),
            pltpu.VMEM((8, slots), F32),
            pltpu.VMEM((8, slots), F32),
            pltpu.VMEM((8, slots), F32),
            pltpu.VMEM((seq_n - 1, 8, slots), F32),
            pltpu.VMEM((8, slots), F32),
            pltpu.VMEM((half - 1, 8, slots), F32),
            pltpu.VMEM((2, 2, half, seq_n) + block, BF16),
            pltpu.VMEM((2, half, seq_n) + block, BF16),
            pltpu.VMEM((2, seq_n, half) + block, BF16),
            pltpu.VMEM((2, seq_n - 1, half) + block, BF16),
            pltpu.VMEM((2, half) + block, BF16),
            pltpu.VMEM((2, half - 1) + block, BF16),
            pltpu.VMEM(block, F32),
            pltpu.VMEM((2, seq_n) + block, BF16),
            pltpu.VMEM((2, seq_n) + block, BF16),
            pltpu.VMEM((2, seq_n - 1) + block, BF16),
            pltpu.VMEM((2, 2, half, seq_n) + block, BF16),
            pltpu.VMEM((2, half, seq_n, owned, 128), F32),
            pltpu.VMEM((2, half, owned, -(-2 * clips // 8) * 8), F32),
            pltpu.VMEM((2, half, owned, -(-seq_n * clips // 8) * 8), F32),
            pltpu.VMEM((2, half, owned, -(-half * clips // 8) * 8), F32),
            pltpu.SemaphoreType.DMA((2 * clips + 2,)),
            pltpu.SemaphoreType.DMA((n_front,)),
            pltpu.SemaphoreType.DMA((n_front,)),
        ],
        compiler_params=pltpu.CompilerParams(collective_id=0, has_side_effects=True),
        name="front",
    )(tokens, router_t, grad_out, w_in, w_out)

    steps = 2 * clips
    t_blocks = steps // clips
    w_blocks = steps // experts
    token_spec = pl.BlockSpec((1, rows // t_blocks, width), lambda i: (i // t_blocks, i % t_blocks, 0))

    def slot_spec(a):
        return pl.BlockSpec((1,) + a.shape[1:], lambda i: (i // t_blocks, 0, 0))

    def fixed(a):
        return pl.BlockSpec(a.shape, lambda i: (0,) * a.ndim)

    mixed, grad_tokens, gr, grad_w_in, grad_w_out = pl.pallas_call(
        functools.partial(finish, clips, steps),
        grid=(steps,),
        out_shape=(
            shape(tokens.shape, BF16),
            shape(tokens.shape, BF16),
            shape((slots, width), F32),
            shape(w_in.shape, BF16),
            shape(w_out.shape, BF16),
        ),
        in_specs=[
            token_spec,
            token_spec,
            slot_spec(so),
            slot_spec(wr),
            fixed(st),
            pl.BlockSpec((1, n_rows, width // w_blocks), lambda i: (i // w_blocks, 0, i % w_blocks)),
            fixed(g),
            pl.BlockSpec((1, n_rows, ff // w_blocks), lambda i: (i // w_blocks, 0, i % w_blocks)),
            fixed(pg),
        ],
        out_specs=(
            token_spec,
            token_spec,
            pl.BlockSpec((slots, width), lambda i: (0, 0)),
            pl.BlockSpec((1, width // w_blocks, ff), lambda i: (i // w_blocks, i % w_blocks, 0)),
            pl.BlockSpec((1, ff // w_blocks, width), lambda i: (i // w_blocks, i % w_blocks, 0)),
        ),
        name="finish",
    )(tokens, grad_out, so, wr, st, x, g, hid, pg)

    out_rows = width // (seq_n * exp_n)
    n_scatter = seq_n * half
    pack = max(1, 128 // slots)
    tile = (out_rows // pack, slots * pack)
    grad_router = pl.pallas_call(
        functools.partial(scatter, seq_n, exp_n),
        out_shape=shape((out_rows, slots), F32),
        in_specs=[vmem],
        out_specs=vmem,
        scratch_shapes=[
            pltpu.VMEM((2, seq_n, half) + tile, BF16),
            pltpu.VMEM((seq_n, half) + tile, BF16),
            pltpu.VMEM((seq_n, half) + tile, BF16),
            pltpu.VMEM((seq_n * half - 1,) + tile, BF16),
            pltpu.SemaphoreType.DMA((n_scatter,)),
            pltpu.SemaphoreType.DMA((n_scatter,)),
        ],
        compiler_params=pltpu.CompilerParams(collective_id=1, has_side_effects=True),
        name="scatter",
    )(gr)
    return mixed, grad_tokens, grad_router, grad_w_in, grad_w_out


def solution(mesh):
    return jax.shard_map(
        functools.partial(on_device, mesh.shape["seq"], mesh.shape["exp"]),
        mesh=mesh,
        in_specs=(
            P(None, ("seq", "exp"), None),
            P(),
            P("exp", None, "seq"),
            P("exp", "seq", None),
            P(None, ("seq", "exp"), None),
        ),
        out_specs=(
            P(None, ("seq", "exp"), None),
            P(None, ("seq", "exp"), None),
            P(("seq", "exp"), None),
            P("exp", None, "seq"),
            P("exp", "seq", None),
        ),
        check_vma=False,
    )
```
